256 devices in a mesh: seq: 64 (over y_hi, x, z), head: 4 (over y_lo, core).
Axes of the slice: x: 4, y: 4 (y_hi: 2, y_lo: 2; y = y_hi * 2 + y_lo), z: 8, core: 2. Of those that a mesh axis runs over, the one named last changes fastest.
Arguments:
- prompt_queries: bfloat16 [12288, 4096], P('seq', 'head'), may hold values from -16 to 16
- prompt_keys: bfloat16 [12288, 1024], P('seq', 'head'), may hold values from -16 to 16
- prompt_values: bfloat16 [12288, 1024], P('seq', 'head'), may hold values from -6 to 6
- span_offset: int32 [64], P('seq'), may hold values from 0 to 63, each once
- appended_queries: bfloat16 [64, 4096], P(None, 'head'), may hold values from -16 to 16
- appended_keys: bfloat16 [64, 1024], P(None, 'head'), may hold values from -6 to 6
- appended_values: bfloat16 [64, 1024], P(None, 'head'), may hold values from -6 to 6
- dec_pos: int32 [64], replicated, may hold values from 2 to 12288, as said below
- out_weight: bfloat16 [4096, 4096], P('head'), may hold values from -0.09375 to 0.09375
Outputs:
- layer_out: bfloat16 [12288, 4096], P(('seq', 'head'))
- dec_out: bfloat16 [64, 4096], P('seq', 'head')
The draws below stay inside these ranges and needn't reach their ends.
Inputs may be any that keep to these rules, and one draw needn't show every extreme that they name: span_offset is a permutation of 0 to 63. `dec_pos`: some appended token stands at 12288 in every draw.
All inputs are finite; a program needn't handle non-finite values.
Results may differ from the reference program's by a relative error of at most 0.015.
Values may be sent and summed in bfloat16 or wider, within the bound.
No kernel may reach another device: no remote copies, remote signals or barrier semaphores. Data moves between devices by JAX's collectives and lax.ppermute only.
A program may use at most 256 MiB of HBM per device.

```python
import math
import jax
import jax.numpy as jnp
from jax import lax

D = 4096
QUERY_HEADS = 32
KEY_VALUE_HEADS = 8
HEAD_SIZE = 128
TOK_DEV = 192
PROMPT_TOKENS = 12288
APPENDED_TOKENS = 64
N_SEQ = 64


def offset_values(key, shape):
    return jnp.clip(jax.random.normal(key, shape, jnp.float32), -6.0, 6.0)


def draw_prompt_queries(key, part):
    base_offset = offset_values(jax.random.fold_in(key, 1), (PROMPT_TOKENS, QUERY_HEADS, HEAD_SIZE))
    return base_offset.reshape(PROMPT_TOKENS, QUERY_HEADS * HEAD_SIZE).astype(jnp.bfloat16)


def draw_prompt_keys(key, part):
    base_offset = offset_values(jax.random.fold_in(key, 2), (PROMPT_TOKENS, KEY_VALUE_HEADS, HEAD_SIZE))
    return base_offset.reshape(PROMPT_TOKENS, KEY_VALUE_HEADS * HEAD_SIZE).astype(jnp.bfloat16)


def draw_appended_queries(key, part):
    base_offset = offset_values(jax.random.fold_in(key, 3), (APPENDED_TOKENS, QUERY_HEADS, HEAD_SIZE))
    return base_offset.reshape(APPENDED_TOKENS, QUERY_HEADS * HEAD_SIZE).astype(jnp.bfloat16)


def draw_dec_pos(key, part):
    top_bit = max(PROMPT_TOKENS.bit_length() - 1, 1)
    powers = jax.random.randint(jax.random.fold_in(key, 4), (APPENDED_TOKENS,), 1, top_bit + 1)
    lowest = jnp.left_shift(jnp.ones((APPENDED_TOKENS,), jnp.int32), powers.astype(jnp.int32))
    extra = jax.random.randint(jax.random.fold_in(key, 5), (APPENDED_TOKENS,), 0, lowest)
    placed = jnp.minimum(lowest + extra, PROMPT_TOKENS)
    row_ids = jnp.arange(APPENDED_TOKENS, dtype=jnp.int32)
    return jnp.where(row_ids == 0, PROMPT_TOKENS, placed).astype(jnp.int32)


def level_of(rng, dims, shards, least, high):
    factor_of = 1.0
    for dim, blocks in shards:
        heights = jax.random.uniform(jax.random.fold_in(jax.random.fold_in(rng, 6), dim), (blocks,), jnp.float32, least / len(shards), high / len(shards))
        factor_of = factor_of * jnp.repeat(jnp.exp(heights), dims[dim] // blocks).reshape((-1,) + (1,) * (len(dims) - 1 - dim))
    return factor_of


def centred(rng, extent, spread, limit, cuts=(), kind=jnp.bfloat16):
    array = jax.random.normal(rng, extent, jnp.float32) * spread
    if len(cuts) > 0:
        array = level_of(rng, extent, cuts, -0.22, 0.18) * array
    return jnp.clip(array, min=-limit, max=limit).astype(kind)


def setup_inputs(seed: int = 0) -> dict:
    arg_keys = jax.random.split(jax.random.key(seed), 10)
    prompt_queries = draw_prompt_queries(jax.random.fold_in(arg_keys[9], 71), 0)
    prompt_keys = draw_prompt_keys(jax.random.fold_in(arg_keys[9], 71), 0)
    prompt_values = centred(arg_keys[2], (PROMPT_TOKENS, KEY_VALUE_HEADS * HEAD_SIZE), 1.0, 6.0, ((0, 64), (1, 4)))
    span_offset = jax.random.permutation(arg_keys[3], N_SEQ).astype(jnp.int32)
    appended_queries = draw_appended_queries(jax.random.fold_in(arg_keys[9], 71), 0)
    appended_keys = centred(arg_keys[5], (APPENDED_TOKENS, KEY_VALUE_HEADS * HEAD_SIZE), 1.0, 6.0, ((1, 4),))
    appended_values = centred(arg_keys[6], (APPENDED_TOKENS, KEY_VALUE_HEADS * HEAD_SIZE), 1.0, 6.0, ((1, 4),))
    dec_pos = draw_dec_pos(jax.random.fold_in(arg_keys[9], 71), 0)
    out_weight = centred(arg_keys[8], (QUERY_HEADS * HEAD_SIZE, D), (QUERY_HEADS * HEAD_SIZE) ** -0.5, 0.09375, ((0, 4),))
    return {"prompt_queries": prompt_queries, "prompt_keys": prompt_keys, "prompt_values": prompt_values, "span_offset": span_offset, "appended_queries": appended_queries, "appended_keys": appended_keys, "appended_values": appended_values, "dec_pos": dec_pos, "out_weight": out_weight}


masked_score = -1e30


def round_trip(values):
    return lax.optimization_barrier(values.astype(jnp.bfloat16)).astype(jnp.float32)


def reference(prompt_queries, prompt_keys, prompt_values, span_offset, appended_queries, appended_keys, appended_values, dec_pos, out_weight):
    group_width = QUERY_HEADS // KEY_VALUE_HEADS
    score_scale = HEAD_SIZE ** -0.5
    slots = jnp.arange(N_SEQ, dtype=jnp.int32)
    inverse = jnp.sum(slots[:, None] * (span_offset[:, None] == slots[None, :]).astype(jnp.int32), axis=0)

    def order_rows(matrix):
        return matrix.reshape(N_SEQ, TOK_DEV, matrix.shape[1])[inverse].reshape(PROMPT_TOKENS, matrix.shape[1])

    queries_ordered = order_rows(prompt_queries).reshape(PROMPT_TOKENS, KEY_VALUE_HEADS, group_width, HEAD_SIZE).transpose(1, 0, 2, 3).astype(jnp.float32)
    keys_ordered = order_rows(prompt_keys).reshape(PROMPT_TOKENS, KEY_VALUE_HEADS, HEAD_SIZE).transpose(1, 0, 2).astype(jnp.float32)
    values_ordered = order_rows(prompt_values).reshape(PROMPT_TOKENS, KEY_VALUE_HEADS, HEAD_SIZE).transpose(1, 0, 2).astype(jnp.float32)
    query_gradient_full = appended_queries.reshape(APPENDED_TOKENS, KEY_VALUE_HEADS, group_width, HEAD_SIZE).transpose(1, 0, 2, 3).astype(jnp.float32)
    key_gradient_full = appended_keys.reshape(APPENDED_TOKENS, KEY_VALUE_HEADS, HEAD_SIZE).transpose(1, 0, 2).astype(jnp.float32)
    value_gradient_full = appended_values.reshape(APPENDED_TOKENS, KEY_VALUE_HEADS, HEAD_SIZE).transpose(1, 0, 2).astype(jnp.float32)
    block = math.gcd(PROMPT_TOKENS, 512)
    positions = jnp.arange(PROMPT_TOKENS, dtype=jnp.int32)

    def one_group(operands):
        q_rows, k_rows, v_rows, dq_rows, dk_rows, dv_rows = operands
        pieces = []
        for number in range(PROMPT_TOKENS // block):
            begin = number * block
            finish = begin + block
            scores = jnp.einsum("rgd,sd->rgs", q_rows[begin:finish], k_rows[:finish]) * score_scale
            allowed = (positions[None, :finish] <= positions[begin:finish, None])[:, None, :]
            row_max = jnp.max(jnp.where(allowed, scores, masked_score), axis=-1, keepdims=True)
            weights = jnp.where(allowed, jnp.exp(scores - row_max), 0.0)
            denominator = jnp.sum(weights, axis=-1, keepdims=True)
            summed = jnp.einsum("rgs,sd->rgd", round_trip(weights), v_rows[:finish])
            pieces.append((summed / denominator).astype(jnp.bfloat16))
        dec_scores = jnp.einsum("rgd,sd->rgs", dq_rows, k_rows) * score_scale
        visible = (positions[None, :] < dec_pos[:, None])[:, None, :]
        self_score = jnp.einsum("rgd,rd->rg", dq_rows, dk_rows) * score_scale
        dec_max = jnp.maximum(jnp.max(jnp.where(visible, dec_scores, masked_score), axis=-1), self_score)
        dec_weights = jnp.where(visible, jnp.exp(dec_scores - dec_max[..., None]), 0.0)
        self_weight = jnp.exp(self_score - dec_max)
        dec_denominator = jnp.sum(dec_weights, axis=-1) + self_weight
        dec_summed = jnp.einsum("rgs,sd->rgd", round_trip(dec_weights), v_rows)
        dec_summed = dec_summed + round_trip(self_weight)[..., None] * dv_rows[:, None, :]
        dec_piece = (dec_summed / dec_denominator[..., None]).astype(jnp.bfloat16)
        return jnp.concatenate(pieces, axis=0), dec_piece

    prompt_attn, dec_attn = lax.map(one_group, (queries_ordered, keys_ordered, values_ordered, query_gradient_full, key_gradient_full, value_gradient_full))
    attn_sorted = prompt_attn.transpose(1, 0, 2, 3).reshape(PROMPT_TOKENS, QUERY_HEADS * HEAD_SIZE)
    attention = attn_sorted.reshape(N_SEQ, TOK_DEV, QUERY_HEADS * HEAD_SIZE)[span_offset].reshape(PROMPT_TOKENS, QUERY_HEADS * HEAD_SIZE)
    layer_out = jnp.dot(attention, out_weight, preferred_element_type=jnp.float32).astype(jnp.bfloat16)
    dec_attention = dec_attn.transpose(1, 0, 2, 3).reshape(APPENDED_TOKENS, QUERY_HEADS * HEAD_SIZE)
    dec_out = jnp.dot(dec_attention, out_weight, preferred_element_type=jnp.float32).astype(jnp.bfloat16)
    return layer_out, dec_out
```

```python
from functools import partial
import math

import jax
import jax.numpy as jnp
from jax import lax
from jax.experimental import pallas as pl
from jax.experimental.pallas import tpu as pltpu
from jax.sharding import Mesh, PartitionSpec as P

HEAD_SIZE = 128
T = 192
TP = T + 8
G = 4
R = G * T
ACC = HEAD_SIZE + 8
NB = 16
LOW = -1e30
SCALE = HEAD_SIZE**-0.5 * math.log2(math.e)


def shift(x, axis, k):
    n = lax.axis_size(axis)
    return lax.ppermute(x, axis, [((i + k) % n, i) for i in range(n)])


def rounded(x):
    return x.astype(jnp.bfloat16).astype(jnp.float32)


def pack_body(idx, q, k, v, kvm, kvo, qm, qo):
    mine = idx[0]
    pos = jnp.full((8, 512), idx[1], jnp.int32).astype(jnp.float32).astype(jnp.bfloat16)
    for kv, qq, head in ((kvm, qm, mine), (kvo, qo, 1 - mine)):
        at = pl.multiple_of(head * HEAD_SIZE, HEAD_SIZE)
        kv[0:T, 0:HEAD_SIZE] = k[:, pl.ds(at, HEAD_SIZE)]
        kv[0:T, HEAD_SIZE:] = v[:, pl.ds(at, HEAD_SIZE)]
        kv[T:TP, :] = pos[:, :256]
        qq[0:T, :] = q[:, pl.ds(pl.multiple_of(head * 512, 512), 512)]
        qq[T:TP, :] = pos


def pack(idx, q, k, v):
    vm = pl.BlockSpec(memory_space=pltpu.VMEM)
    return pl.pallas_call(
        pack_body,
        in_specs=[pl.BlockSpec(memory_space=pltpu.SMEM), vm, vm, vm],
        out_specs=[vm] * 4,
        out_shape=[jax.ShapeDtypeStruct((TP, w), jnp.bfloat16) for w in (256, 256, 512, 512)],
        name="pack",
    )(idx, q, k, v)


def dec_step(q, blocks, acc, top, total):
    scores = []
    high = top
    for k, _, seen in blocks:
        s = lax.dot_general(
            q, k, (((1,), (1,)), ((), ())), preferred_element_type=jnp.float32
        )
        s = jnp.where(seen, s * SCALE, LOW)
        scores.append(s)
        high = jnp.maximum(high, rounded(jnp.max(s, axis=1, keepdims=True)))
    factor = jnp.exp2(top - high)
    total, acc = total * factor, acc * factor
    for s, (_, v, seen) in zip(scores, blocks):
        w = jnp.where(seen, jnp.exp2(s - high), 0.0)
        total = total + jnp.sum(w, axis=1, keepdims=True)
        acc = acc + jnp.dot(w.astype(jnp.bfloat16), v, preferred_element_type=jnp.float32)
    return acc, high, total


def sort_blocks(pieces, kv, table, limit):
    keys = lax.broadcasted_iota(jnp.int32, (32, T), 1)
    where = []
    for ref in pieces:
        for at in (0, TP):
            tag = ref[at + T : at + TP, 0:128].astype(jnp.float32)
            where.append((ref, at, jnp.max(tag).astype(jnp.int32)))
    blocks = []
    for ref, at, pos in where:
        rank = sum((other < pos).astype(jnp.int32) for _, _, other in where)
        block = ref[at : at + T, :]
        kv[pl.ds(pl.multiple_of(rank * T, T), T), :] = block
        table[rank] = pos
        blocks.append((block[:, :HEAD_SIZE], block[:, HEAD_SIZE:], keys + pos * T < limit))
    return blocks


def gather_body(dq, sk, sv, dpos, *refs):
    pieces, (kv, table, dec) = refs[:-3], refs[-3:]
    q = dq[...]
    blocks = sort_blocks(pieces, kv, table, dpos[:, 0:1])
    own = lax.broadcasted_iota(jnp.int32, (32, 1), 0) < 8
    score = jnp.sum(q.astype(jnp.float32) * sk[...].astype(jnp.float32), axis=1, keepdims=True)
    score = jnp.where(own, score * SCALE, LOW)
    top = rounded(score)
    weight = jnp.where(own, jnp.exp2(score - top), 0.0)
    acc = rounded(weight) * sv[...].astype(jnp.float32)
    acc, top, total = dec_step(q, blocks, acc, top, weight)
    rows = lax.broadcasted_iota(jnp.int32, (8, R), 0)
    top = jnp.broadcast_to(top, (32, HEAD_SIZE))
    total = jnp.broadcast_to(total, (32, HEAD_SIZE))
    for n in range(8):

        def row(a):
            parts = [a[n * G + h : n * G + h + 1, :] for h in range(G)]
            flat = jnp.concatenate(parts + [jnp.zeros((1, 256), jnp.float32)], axis=1)
            return jnp.broadcast_to(flat, (8, R))

        tile = jnp.where(rows == 2, row(acc), 0.0)
        tile = jnp.where(rows == 3, row(top), tile)
        tile = jnp.where(rows == 4, row(total), tile)
        dec[n] = tile


def gather(small, pieces):
    vm = pl.BlockSpec(memory_space=pltpu.VMEM)
    return pl.pallas_call(
        gather_body,
        in_specs=[vm] * (len(small) + len(pieces)),
        out_specs=[vm, pl.BlockSpec(memory_space=pltpu.SMEM), vm],
        out_shape=[
            jax.ShapeDtypeStruct((NB * T, 256), jnp.bfloat16),
            jax.ShapeDtypeStruct((NB,), jnp.int32),
            jax.ShapeDtypeStruct((8, 8, R), jnp.float32),
        ],
        name="gather",
    )(*small, *pieces)


W = 256
SPREAD = 60.0


def attend_body(groups, table, *refs):
    n = len(groups)
    queries, (kv, dec, out, qs, acc, stat, positions, again) = refs[:n], refs[n:]
    for i, q in enumerate(queries):
        for b in range(2):
            at = b * TP
            for h in range(G):
                qs[2 * i + b, h * T : (h + 1) * T, :] = q[
                    at : at + T, h * HEAD_SIZE : (h + 1) * HEAD_SIZE
                ]
            tag = q[at + T : at + TP, 0:128].astype(jnp.float32)
            positions[2 * i + b] = jnp.max(tag).astype(jnp.int32)
    rows = lax.broadcasted_iota(jnp.int32, (8, R), 0)
    cols = list(range(0, R, W))

    @pl.loop(0, 2 * n)
    def _(turn):
        pos = positions[turn]
        count = jnp.int32(0)
        same = jnp.int32(0)
        for m in range(NB):
            count = count + (table[m] < pos).astype(jnp.int32)
            same = same + (table[m] == pos).astype(jnp.int32)
        rest = count + same

        def read(first, blocks):
            at = pl.multiple_of(first * T, T)
            k = kv[pl.ds(at, blocks * T), 0:HEAD_SIZE]
            v = kv[pl.ds(at, blocks * T), HEAD_SIZE:]
            scores = [
                lax.dot_general(
                    k,
                    qs[turn, c : c + W, :],
                    (((1,), (1,)), ((), ())),
                    preferred_element_type=jnp.float32,
                )
                for c in cols
            ]
            return v, scores

        def apply(v, w):
            return lax.dot_general(
                v,
                w.astype(jnp.bfloat16),
                (((0,), (0,)), ((), ())),
                preferred_element_type=jnp.float32,
            )

        def exact(first):
            v, scores = read(first, 2)
            for c, s in zip(cols, scores):
                row = lax.broadcasted_iota(jnp.int32, (1, W), 1) + c
                for edge in (3 * T, 2 * T, T):
                    row = jnp.where(row >= edge, row - edge, row)
                limit = jnp.where(same > 0, row, -1) + (count - first) * T
                key = lax.broadcasted_iota(jnp.int32, (2 * T, W), 0)
                s = jnp.where(key <= limit, s * SCALE, LOW)
                old = stat[0:1, c : c + W]
                high = jnp.maximum(old, rounded(jnp.max(s, axis=0, keepdims=True)))
                factor = jnp.exp2(old - high)
                w = jnp.exp2(s - high)
                stat[0:1, c : c + W] = high
                stat[1:2, c : c + W] = stat[1:2, c : c + W] * factor + jnp.sum(
                    w, axis=0, keepdims=True
                )
                acc[:, c : c + W] = acc[:, c : c + W] * factor + apply(v, w)

        def quick(first):
            v, scores = read(first, 4)
            for c, s in zip(cols, scores):
                s = s * SCALE
                w = jnp.exp2(s - stat[0:1, c : c + W])
                stat[2:3, c : c + W] = jnp.maximum(
                    stat[2:3, c : c + W], jnp.max(s, axis=0, keepdims=True)
                )
                stat[1:2, c : c + W] = stat[1:2, c : c + W] + jnp.sum(w, axis=0, keepdims=True)
                acc[:, c : c + W] = acc[:, c : c + W] + apply(v, w)

        again[0] = jnp.int32(1)

        @pl.loop(0, 2)
        def _(attempt):
            @pl.when(again[0] == 1)
            def _():
                fours = jnp.where(attempt == 0, jnp.maximum(rest - 1, 0) // 4, 0)
                acc[...] = jnp.zeros_like(acc)
                stat[...] = jnp.where(rows == 1, 0.0, LOW)

                @pl.loop(0, (rest - 4 * fours + 1) // 2)
                def _(i):
                    exact(4 * fours + 2 * i)

                @pl.loop(0, fours)
                def _(i):
                    quick(4 * i)

                over = jnp.max(stat[2:3, :] - stat[0:1, :]) > SPREAD
                again[0] = over.astype(jnp.int32)

        out[turn, 0:HEAD_SIZE, :] = acc[...].astype(jnp.bfloat16)
        tile = jnp.where(rows < 2, stat[...], dec_tile(dec, groups, turn))
        out[turn, HEAD_SIZE:, :] = tile.astype(jnp.bfloat16)


def dec_tile(dec, groups, turn):
    number = jnp.int32(0)
    for i, g in enumerate(groups):
        number = jnp.where(turn // 2 == i, 2 * g + turn % 2, number)
    return dec[number]


def attend(table, queries, kv, dec, groups):
    n = len(groups)
    vm = pl.BlockSpec(memory_space=pltpu.VMEM)
    return pl.pallas_call(
        partial(attend_body, groups),
        in_specs=[pl.BlockSpec(memory_space=pltpu.SMEM)] + [vm] * (n + 2),
        out_specs=vm,
        out_shape=jax.ShapeDtypeStruct((2 * n, ACC, R), jnp.bfloat16),
        scratch_shapes=[
            pltpu.VMEM((2 * n, R, HEAD_SIZE), jnp.bfloat16),
            pltpu.VMEM((HEAD_SIZE, R), jnp.float32),
            pltpu.VMEM((8, R), jnp.float32),
            pltpu.SMEM((2 * n,), jnp.int32),
            pltpu.SMEM((1,), jnp.int32),
        ],
        cost_estimate=pl.CostEstimate(
            flops=2 * n * NB * T * R * HEAD_SIZE * 4,
            bytes_accessed=4 << 20,
            transcendentals=2 * n * NB * T * R,
        ),
        name="attend",
    )(table, *queries, kv, dec)


def merge_body(core, *refs):
    parts, outs, turned = refs[:4], refs[4:8], refs[8]
    for b in range(2):
        stats = [p[b, HEAD_SIZE:, :].astype(jnp.float32) for p in parts]
        high = stats[0][0:1, :]
        for s in stats[1:]:
            high = jnp.maximum(high, s[0:1, :])
        factors = [jnp.exp2(s[0:1, :] - high) for s in stats]
        total = sum(f * s[1:2, :] for f, s in zip(factors, stats))
        acc = sum(
            f * p[b, 0:HEAD_SIZE, :].astype(jnp.float32) for f, p in zip(factors, parts)
        )
        flat = acc / total
        for h in range(G):
            head = flat[:, h * T : (h + 1) * T].T
            turned[:, h * HEAD_SIZE : (h + 1) * HEAD_SIZE] = head.astype(jnp.bfloat16)
        high = stats[0][3:4, :512]
        for s in stats[1:]:
            high = jnp.maximum(high, s[3:4, :512])
        factors = [jnp.exp2(s[3:4, :512] - high) for s in stats]
        total = sum(f * s[4:5, :512] for f, s in zip(factors, stats))
        acc = sum(f * s[2:3, :512] for f, s in zip(factors, stats))
        row = jnp.broadcast_to(acc / total, (8, 512)).astype(jnp.bfloat16)
        for other in range(2):
            out = outs[2 * b + other]
            start = core[0] * 48 if other == 0 else (1 - core[0]) * 48
            for half in range(2):
                rows = pl.ds(pl.multiple_of(start + 96 * half, 16), 48)
                out[half * 48 : half * 48 + 48, :] = turned[rows, :]
            out[96:104, :] = row


def merge(core, parts):
    vm = pl.BlockSpec(memory_space=pltpu.VMEM)
    return pl.pallas_call(
        merge_body,
        in_specs=[pl.BlockSpec(memory_space=pltpu.SMEM)] + [vm] * 4,
        out_specs=[vm] * 4,
        out_shape=[jax.ShapeDtypeStruct((104, 512), jnp.bfloat16)] * 4,
        scratch_shapes=[pltpu.VMEM((T, 512), jnp.bfloat16)],
        name="merge",
    )(core, *parts)


def on_device(q, k, v, span_offset, appended_q, appended_k, appended_v, dec_pos, out_weight):
    yh, x, z = (lax.axis_index(a) for a in ("yh", "x", "z"))
    yl, c = lax.axis_index("yl"), lax.axis_index("c")
    idx = jnp.stack([yh.astype(jnp.int32), span_offset[0]])
    kv_mine, kv_other, q_mine, q_other = pack(idx, q, k, v)
    kv_pair = jnp.concatenate([kv_mine, shift(kv_other, "yh", 1)], axis=0)
    q_pair = jnp.concatenate([q_mine, shift(q_other, "yh", 1)], axis=0)

    f1, b1 = shift(kv_pair, "z", 1), shift(kv_pair, "z", -1)
    f2, b2 = shift(f1, "z", 1), shift(b1, "z", -1)
    f3, b3 = shift(f2, "z", 1), shift(b2, "z", -1)
    f4 = shift(f3, "z", 1)
    groups = [q_pair, shift(q_pair, "x", 1), shift(q_pair, "x", 2), shift(q_pair, "x", -1)]
    other_weight = shift(out_weight, "c", 1)

    tokens = jnp.stack(
        [
            jnp.bitwise_xor(yh, b) * 32 + ((x + g) % 4) * 8 + z
            for g in range(4)
            for b in range(2)
        ]
    ).astype(jnp.int32)
    pick = (tokens[:, None] == jnp.arange(64, dtype=jnp.int32)[None, :]).astype(jnp.bfloat16)

    def rows_of(a):
        w = a.shape[1] // 2
        a = jnp.where(yh == 0, a[:, :w], a[:, w:])
        return jnp.dot(pick, a, preferred_element_type=jnp.float32).astype(jnp.bfloat16)

    dq = rows_of(appended_q).reshape(32, HEAD_SIZE)
    sk = jnp.repeat(rows_of(appended_k), G, axis=0)
    sv = jnp.repeat(rows_of(appended_v), G, axis=0)
    dpos = jnp.sum(jnp.where(tokens[:, None] == jnp.arange(64)[None, :], dec_pos[None, :], 0), axis=1)
    dpos = jnp.broadcast_to(jnp.repeat(dpos, G)[:, None], (32, 128)).astype(jnp.int32)

    kv, table, dec = gather([dq, sk, sv, dpos], [kv_pair, f1, b1, f2, b2, f3, b3, f4])
    far = attend(table, [groups[2]], kv, dec, [2])
    table, far = lax.optimization_barrier((table, far))
    back2 = shift(far, "x", 2)
    near = attend(table, [groups[1], groups[3]], kv, dec, [1, 3])
    table, near = lax.optimization_barrier((table, near))
    back1 = shift(near[:2], "x", -1)
    back3 = shift(near[2:], "x", 1)
    own = attend(table, [groups[0]], kv, dec, [0])

    mine, by_core, by_pair, by_both = merge(
        c.astype(jnp.int32)[None], [own, back1, back2, back3]
    )
    by_core = shift(by_core, "c", 1)
    by_pair = shift(by_pair, "yh", 1)
    by_both = lax.ppermute(by_both, ("yh", "c"), [(i, 3 - i) for i in range(4)])
    first = yh == 0

    def ordered(a, b):
        return jnp.concatenate([jnp.where(first, a, b), jnp.where(first, b, a)], axis=1)

    here, there = ordered(mine, by_pair), ordered(by_core, by_both)
    result = jnp.dot(here, out_weight, preferred_element_type=jnp.float32)
    result = result + jnp.dot(there, other_weight, preferred_element_type=jnp.float32)
    low, high, tail = result[:48], result[48:96], result[96:]
    low_here = yl == 0
    send = jnp.where(low_here, high, low)
    keep = jnp.where(low_here, low, high)
    arrived = shift(jnp.concatenate([send, tail], axis=0).astype(jnp.bfloat16), "yl", 1)
    layer_out = (keep + arrived[:48].astype(jnp.float32)).astype(jnp.bfloat16)
    tail = tail[0] + arrived[48].astype(jnp.float32)
    dec_out = lax.dynamic_slice_in_dim(tail, (yl * 2 + c) * 1024, 1024)[None]
    return layer_out, dec_out.astype(jnp.bfloat16)


def solution(mesh):
    fine = Mesh(mesh.devices.reshape(2, 4, 8, 2, 2), ("yh", "x", "z", "yl", "c"))
    seq, head = ("yh", "x", "z"), ("yl", "c")
    in_specs = (
        P(seq, head),
        P(seq, head),
        P(seq, head),
        P(seq),
        P(None, head),
        P(None, head),
        P(None, head),
        P(),
        P(head, None),
    )
    out_specs = (P(seq + head, None), P(seq, head))
    return jax.shard_map(on_device, mesh=fine, in_specs=in_specs, out_specs=out_specs, check_vma=False)
```

```python
from functools import partial
import math

import jax
import jax.numpy as jnp
from jax import lax
from jax.experimental import pallas as pl
from jax.experimental.pallas import tpu as pltpu
from jax.sharding import Mesh, PartitionSpec as P


HEAD_SIZE = 128
T = 192
TP = T + 8
G = 4
R = G * T
ACC = HEAD_SIZE + 8
NB = 16
LOW = -1e30
EMPTY = -1e29
SCALE = HEAD_SIZE**-0.5 * math.log2(math.e)


def shift(x, axis, k):
    n = lax.axis_size(axis)
    return lax.ppermute(x, axis, [((i + k) % n, i) for i in range(n)])


def rounded(x):
    return x.astype(jnp.bfloat16).astype(jnp.float32)


def spec(space=pltpu.VMEM):
    return pl.BlockSpec(memory_space=space)


def params():
    return pltpu.CompilerParams(vmem_limit_bytes=24 << 20)


def position_tile(offset, width):
    return jnp.full((8, width), offset[0], jnp.int32).astype(jnp.float32).astype(jnp.bfloat16)


def pack_kv_body(offset, k, v, mine, other):
    yh = lax.axis_index("yh")
    tile = position_tile(offset, 256)
    for out, head in ((mine, yh), (other, 1 - yh)):
        at = pl.multiple_of(head * HEAD_SIZE, HEAD_SIZE)
        out[0:T, 0:HEAD_SIZE] = k[:, pl.ds(at, HEAD_SIZE)]
        out[0:T, HEAD_SIZE:] = v[:, pl.ds(at, HEAD_SIZE)]
        out[T:TP, :] = tile


def pack_q_body(offset, q, mine, other):
    yh = lax.axis_index("yh")
    tile = position_tile(offset, 512)
    for out, head in ((mine, yh), (other, 1 - yh)):
        out[0:T, :] = q[:, pl.ds(pl.multiple_of(head * 512, 512), 512)]
        out[T:TP, :] = tile


def pack(body, width, offset, *arrays):
    return pl.pallas_call(
        body,
        in_specs=[spec(pltpu.SMEM)] + [spec()] * len(arrays),
        out_specs=[spec()] * 2,
        out_shape=[jax.ShapeDtypeStruct((TP, width), jnp.bfloat16)] * 2,
        compiler_params=params(),
        name="pack",
    )(offset, *arrays)


def dec_step(q, blocks, acc, top, total):
    scores = []
    high = top
    for k, _, seen in blocks:
        s = lax.dot_general(
            q, k, (((1,), (1,)), ((), ())), preferred_element_type=jnp.float32
        )
        s = jnp.where(seen, s * SCALE, LOW)
        scores.append(s)
        high = jnp.maximum(high, rounded(jnp.max(s, axis=1, keepdims=True)))
    factor = jnp.exp2(top - high)
    total, acc = total * factor, acc * factor
    for s, (_, v, seen) in zip(scores, blocks):
        w = jnp.where(seen, jnp.exp2(s - high), 0.0)
        total = total + jnp.sum(w, axis=1, keepdims=True)
        acc = acc + jnp.dot(w.astype(jnp.bfloat16), v, preferred_element_type=jnp.float32)
    return acc, high, total


def sort_blocks(pieces, kv, table, limit):
    keys = lax.broadcasted_iota(jnp.int32, (32, T), 1)
    where = []
    for ref in pieces:
        for at in (0, TP):
            tag = ref[at + T : at + TP, 0:128].astype(jnp.float32)
            where.append((ref, at, jnp.max(tag).astype(jnp.int32)))
    blocks = []
    for ref, at, pos in where:
        rank = sum((other < pos).astype(jnp.int32) for _, _, other in where)
        block = ref[at : at + T, :]
        kv[pl.ds(pl.multiple_of(rank * T, T), T), :] = block
        table[rank] = pos
        blocks.append((block[:, :HEAD_SIZE], block[:, HEAD_SIZE:], keys + pos * T < limit))
    return blocks


def early_body(dq, sk, sv, dpos, *refs):
    pieces, state = refs[:-1], refs[-1]
    q = dq[...]
    limit = dpos[:, 0:1]
    keys = lax.broadcasted_iota(jnp.int32, (32, T), 1)
    blocks = []
    for ref in pieces:
        for at in (0, TP):
            pos = ref[at + T : at + T + 1, 0:1].astype(jnp.float32).astype(jnp.int32)
            block = ref[at : at + T, :]
            blocks.append((block[:, :HEAD_SIZE], block[:, HEAD_SIZE:], keys + pos * T < limit))
    own = lax.broadcasted_iota(jnp.int32, (32, 1), 0) < 8
    score = jnp.sum(q.astype(jnp.float32) * sk[...].astype(jnp.float32), axis=1, keepdims=True)
    score = jnp.where(own, score * SCALE, LOW)
    top = rounded(score)
    weight = jnp.where(own, jnp.exp2(score - top), 0.0)
    acc = rounded(weight) * sv[...].astype(jnp.float32)
    acc, top, total = dec_step(q, blocks, acc, top, weight)
    state[0:32, :] = acc
    state[32:64, :] = jnp.broadcast_to(top, (32, HEAD_SIZE))
    state[64:96, :] = jnp.broadcast_to(total, (32, HEAD_SIZE))


def early(small, pieces):
    return pl.pallas_call(
        early_body,
        in_specs=[spec()] * (len(small) + len(pieces)),
        out_specs=spec(),
        out_shape=jax.ShapeDtypeStruct((96, HEAD_SIZE), jnp.float32),
        compiler_params=params(),
        name="early",
    )(*small, *pieces)


def gather_body(early_blocks, dq, state, dpos, *refs):
    pieces, (kv, table, dec) = refs[:-3], refs[-3:]
    blocks = sort_blocks(pieces, kv, table, dpos[:, 0:1])[early_blocks:]
    acc, top, total = dec_step(
        dq[...], blocks, state[0:32, :], state[32:64, 0:1], state[64:96, 0:1]
    )
    rows = lax.broadcasted_iota(jnp.int32, (8, R), 0)
    top = jnp.broadcast_to(top, (32, HEAD_SIZE))
    total = jnp.broadcast_to(total, (32, HEAD_SIZE))
    for n in range(8):

        def row(a):
            parts = [a[n * G + h : n * G + h + 1, :] for h in range(G)]
            flat = jnp.concatenate(parts + [jnp.zeros((1, 256), jnp.float32)], axis=1)
            return jnp.broadcast_to(flat, (8, R))

        tile = jnp.where(rows == 2, row(acc), 0.0)
        tile = jnp.where(rows == 3, row(top), tile)
        tile = jnp.where(rows == 4, row(total), tile)
        dec[n] = tile


def gather(early_blocks, small, pieces):
    return pl.pallas_call(
        partial(gather_body, early_blocks),
        in_specs=[spec()] * (len(small) + len(pieces)),
        out_specs=[spec(), spec(pltpu.SMEM), spec()],
        out_shape=[
            jax.ShapeDtypeStruct((NB * T, 256), jnp.bfloat16),
            jax.ShapeDtypeStruct((NB,), jnp.int32),
            jax.ShapeDtypeStruct((8, 8, R), jnp.float32),
        ],
        compiler_params=params(),
        name="gather",
    )(*small, *pieces)


W = 256
SPREAD = 60.0


def attend_body(groups, table, *refs):
    n = len(groups)
    queries, (kv, dec), outs = refs[:n], refs[n : n + 2], refs[n + 2 : 2 * n + 2]
    qs, acc, stat, positions, again = refs[2 * n + 2 :]
    for i, q in enumerate(queries):
        for b in range(2):
            at = b * TP
            for h in range(G):
                qs[2 * i + b, h * T : (h + 1) * T, :] = q[
                    at : at + T, h * HEAD_SIZE : (h + 1) * HEAD_SIZE
                ]
            tag = q[at + T : at + TP, 0:128].astype(jnp.float32)
            positions[2 * i + b] = jnp.max(tag).astype(jnp.int32)
    rows = lax.broadcasted_iota(jnp.int32, (8, R), 0)
    cols = list(range(0, R, W))

    @pl.loop(0, n)
    def _(turn):
        counts, sames = [], []
        for b in range(2):
            pos = positions[2 * turn + b]
            count = jnp.int32(0)
            same = jnp.int32(0)
            for m in range(NB):
                count = count + (table[m] < pos).astype(jnp.int32)
                same = same + (table[m] == pos).astype(jnp.int32)
            counts.append(count)
            sames.append(same)
        rests = [c + s for c, s in zip(counts, sames)]

        def read(first, blocks, b):
            at = pl.multiple_of(first * T, T)
            k = kv[pl.ds(at, blocks * T), 0:HEAD_SIZE]
            v = kv[pl.ds(at, blocks * T), HEAD_SIZE:]
            scores = [
                lax.dot_general(
                    k,
                    qs[2 * turn + b, c : c + W, :],
                    (((1,), (1,)), ((), ())),
                    preferred_element_type=jnp.float32,
                )
                for c in cols
            ]
            return v, scores

        def apply(v, w):
            return lax.dot_general(
                v,
                w.astype(jnp.bfloat16),
                (((0,), (0,)), ((), ())),
                preferred_element_type=jnp.float32,
            )

        def exact(fours, i):
            reads = []
            for b in range(2):
                first = jnp.minimum(4 * fours[b] + 2 * i, NB - 2)
                live = 4 * fours[b] + 2 * i < rests[b]
                seen = jnp.where(live, (counts[b] - first) * T, -2 * NB * T)
                reads.append((seen, *read(first, 2, b)))
            for n, c in enumerate(cols):
                row = lax.broadcasted_iota(jnp.int32, (1, W), 1) + c
                for edge in (3 * T, 2 * T, T):
                    row = jnp.where(row >= edge, row - edge, row)
                key = lax.broadcasted_iota(jnp.int32, (2 * T, W), 0)
                for b, (seen, v, scores) in enumerate(reads):
                    limit = jnp.where(sames[b] > 0, row, -1) + seen
                    s = jnp.where(key <= limit, scores[n] * SCALE, LOW)
                    old = stat[b, 0:1, c : c + W]
                    high = jnp.maximum(old, rounded(jnp.max(s, axis=0, keepdims=True)))
                    factor = jnp.exp2(old - high)
                    w = jnp.exp2(s - high)
                    stat[b, 0:1, c : c + W] = high
                    stat[b, 1:2, c : c + W] = stat[b, 1:2, c : c + W] * factor + jnp.sum(
                        w, axis=0, keepdims=True
                    )
                    acc[b, :, c : c + W] = acc[b, :, c : c + W] * factor + apply(v, w)

        def quick(first, which):
            reads = [(b, *read(first, 4, b)) for b in which]
            for n, c in enumerate(cols):
                for b, v, scores in reads:
                    s = scores[n] * SCALE
                    w = jnp.exp2(s - stat[b, 0:1, c : c + W])
                    stat[b, 2:3, c : c + W] = jnp.maximum(
                        stat[b, 2:3, c : c + W], jnp.max(s, axis=0, keepdims=True)
                    )
                    stat[b, 1:2, c : c + W] = stat[b, 1:2, c : c + W] + jnp.sum(
                        w, axis=0, keepdims=True
                    )
                    acc[b, :, c : c + W] = acc[b, :, c : c + W] + apply(v, w)

        again[0] = jnp.int32(1)

        @pl.loop(0, 2)
        def _(attempt):
            @pl.when(again[0] == 1)
            def _():
                fours = [
                    jnp.where(attempt == 0, jnp.maximum(rest - 1, 0) // 4, 0) for rest in rests
                ]
                acc[...] = jnp.zeros_like(acc)
                for b in range(2):
                    stat[b] = jnp.where(rows == 1, 0.0, EMPTY)
                left = [(rest - 4 * f + 1) // 2 for rest, f in zip(rests, fours)]

                @pl.loop(0, jnp.maximum(left[0], left[1]))
                def _(i):
                    exact(fours, i)

                both = jnp.minimum(fours[0], fours[1])
                longer = (fours[1] > fours[0]).astype(jnp.int32)

                @pl.loop(0, both)
                def _(i):
                    quick(4 * i, (0, 1))

                @pl.loop(both, jnp.maximum(fours[0], fours[1]))
                def _(i):
                    quick(4 * i, (longer,))

                over = jnp.maximum(
                    jnp.max(stat[0, 2:3, :] - stat[0, 0:1, :]),
                    jnp.max(stat[1, 2:3, :] - stat[1, 0:1, :]),
                )
                again[0] = (over > SPREAD).astype(jnp.int32)

        for i, (out, group) in enumerate(zip(outs, groups)):

            @pl.when(turn == i)
            def _():
                for b in range(2):
                    out[b, 0:HEAD_SIZE, :] = acc[b].astype(jnp.bfloat16)
                    tile = jnp.where(rows < 2, stat[b], dec[2 * group + b])
                    out[b, HEAD_SIZE:, :] = tile.astype(jnp.bfloat16)


def attend_call(table, queries, kv, dec, groups):
    n = len(groups)
    return pl.pallas_call(
        partial(attend_body, groups),
        in_specs=[spec(pltpu.SMEM)] + [spec()] * (n + 2),
        out_specs=[spec()] * n,
        out_shape=[jax.ShapeDtypeStruct((2, ACC, R), jnp.bfloat16)] * n,
        scratch_shapes=[
            pltpu.VMEM((2 * n, R, HEAD_SIZE), jnp.bfloat16),
            pltpu.VMEM((2, HEAD_SIZE, R), jnp.float32),
            pltpu.VMEM((2, 8, R), jnp.float32),
            pltpu.SMEM((2 * n,), jnp.int32),
            pltpu.SMEM((1,), jnp.int32),
        ],
        cost_estimate=pl.CostEstimate(
            flops=2 * n * NB * T * R * HEAD_SIZE * 4,
            bytes_accessed=4 << 20,
            transcendentals=2 * n * NB * T * R,
        ),
        compiler_params=params(),
        name="attend",
    )(table, *queries, kv, dec)


def merge_body(*refs):
    core = lax.axis_index("c")
    parts, outs, turned = refs[:4], refs[4:8], refs[8]
    for b in range(2):
        stats = [p[b, HEAD_SIZE:, :].astype(jnp.float32) for p in parts]
        high = stats[0][0:1, :]
        for s in stats[1:]:
            high = jnp.maximum(high, s[0:1, :])
        factors = [jnp.exp2(s[0:1, :] - high) for s in stats]
        total = sum(f * s[1:2, :] for f, s in zip(factors, stats))
        acc = sum(
            f * p[b, 0:HEAD_SIZE, :].astype(jnp.float32) for f, p in zip(factors, parts)
        )
        flat = acc / total
        for h in range(G):
            head = flat[:, h * T : (h + 1) * T].T
            turned[:, h * HEAD_SIZE : (h + 1) * HEAD_SIZE] = head.astype(jnp.bfloat16)
        high = stats[0][3:4, :512]
        for s in stats[1:]:
            high = jnp.maximum(high, s[3:4, :512])
        factors = [jnp.exp2(s[3:4, :512] - high) for s in stats]
        total = sum(f * s[4:5, :512] for f, s in zip(factors, stats))
        acc = sum(f * s[2:3, :512] for f, s in zip(factors, stats))
        row = jnp.broadcast_to(acc / total, (8, 512)).astype(jnp.bfloat16)
        for other in range(2):
            out = outs[2 * b + other]
            start = core * 48 if other == 0 else (1 - core) * 48
            for half in range(2):
                rows = pl.ds(pl.multiple_of(start + 96 * half, 16), 48)
                out[half * 48 : half * 48 + 48, :] = turned[rows, :]
            out[96:104, :] = row


def merge(parts):
    return pl.pallas_call(
        merge_body,
        in_specs=[spec()] * 4,
        out_specs=[spec()] * 4,
        out_shape=[jax.ShapeDtypeStruct((104, 512), jnp.bfloat16)] * 4,
        scratch_shapes=[pltpu.VMEM((T, 512), jnp.bfloat16)],
        compiler_params=params(),
        name="merge",
    )(*parts)


def layer(q, k, v, span_offset, appended_q, appended_k, appended_v, dec_pos, out_weight):
    yh, x, z = (lax.axis_index(a) for a in ("yh", "x", "z"))
    yl, c = lax.axis_index("yl"), lax.axis_index("c")
    kv_mine, kv_other = pack(pack_kv_body, 256, span_offset, k, v)
    q_mine, q_other = pack(pack_q_body, 512, span_offset, q)
    kv_pair = jnp.concatenate([kv_mine, shift(kv_other, "yh", 1)], axis=0)
    q_pair = jnp.concatenate([q_mine, shift(q_other, "yh", 1)], axis=0)

    other_weight = shift(out_weight, "c", 1)

    tokens = jnp.stack(
        [
            jnp.bitwise_xor(yh, b) * 32 + ((x + g) % 4) * 8 + z
            for g in range(4)
            for b in range(2)
        ]
    ).astype(jnp.int32)
    pick = (tokens[:, None] == jnp.arange(64, dtype=jnp.int32)[None, :]).astype(jnp.bfloat16)

    def rows_of(a):
        w = a.shape[1] // 2
        a = jnp.where(yh == 0, a[:, :w], a[:, w:])
        return jnp.dot(pick, a, preferred_element_type=jnp.float32).astype(jnp.bfloat16)

    dq = rows_of(appended_q).reshape(32, HEAD_SIZE)
    sk = jnp.repeat(rows_of(appended_k), G, axis=0)
    sv = jnp.repeat(rows_of(appended_v), G, axis=0)
    dpos = jnp.sum(jnp.where(tokens[:, None] == jnp.arange(64)[None, :], dec_pos[None, :], 0), axis=1)
    dpos = jnp.broadcast_to(jnp.repeat(dpos, G)[:, None], (32, 128)).astype(jnp.int32)

    f1, b1 = shift(kv_pair, "z", 1), shift(kv_pair, "z", -1)
    f1, b1, dq, sk, sv, dpos = lax.optimization_barrier((f1, b1, dq, sk, sv, dpos))
    f2, b2 = shift(f1, "z", 1), shift(b1, "z", -1)
    groups = [q_pair, shift(q_pair, "x", 1), shift(q_pair, "x", 2), shift(q_pair, "x", -1)]
    state = early([dq, sk, sv, dpos], [kv_pair, f1, b1])
    f3, b3 = shift(f2, "z", 1), shift(b2, "z", -1)
    f4 = shift(f3, "z", 1)
    kv, table, dec = gather(6, [dq, state, dpos], [kv_pair, f1, b1, f2, b2, f3, b3, f4])
    table, other_weight = lax.optimization_barrier((table, other_weight))
    (far,) = attend_call(table, [groups[2]], kv, dec, [2])
    table, far = lax.optimization_barrier((table, far))
    back2 = shift(far, "x", 2)
    ahead, behind = attend_call(table, [groups[1], groups[3]], kv, dec, [1, 3])
    table, ahead, behind = lax.optimization_barrier((table, ahead, behind))
    back1 = shift(ahead, "x", -1)
    back3 = shift(behind, "x", 1)
    (own,) = attend_call(table, [groups[0]], kv, dec, [0])

    mine, by_core, by_pair, by_both = merge([own, back1, back2, back3])
    by_core = shift(by_core, "c", 1)
    by_pair = shift(by_pair, "yh", 1)
    by_both = lax.ppermute(by_both, ("yh", "c"), [(i, 3 - i) for i in range(4)])
    first = yh == 0

    def ordered(a, b):
        return jnp.concatenate([jnp.where(first, a, b), jnp.where(first, b, a)], axis=1)

    here, there = ordered(mine, by_pair), ordered(by_core, by_both)
    result = jnp.dot(here, out_weight, preferred_element_type=jnp.float32)
    result = result + jnp.dot(there, other_weight, preferred_element_type=jnp.float32)
    low, high, tail = result[:48], result[48:96], result[96:]
    low_here = yl == 0
    send = jnp.where(low_here, high, low)
    keep = jnp.where(low_here, low, high)
    arrived = shift(jnp.concatenate([send, tail], axis=0).astype(jnp.bfloat16), "yl", 1)
    layer_out = (keep + arrived[:48].astype(jnp.float32)).astype(jnp.bfloat16)
    tail = tail[0] + arrived[48].astype(jnp.float32)
    dec_out = lax.dynamic_slice_in_dim(tail, (yl * 2 + c) * 1024, 1024)[None]
    return layer_out, dec_out.astype(jnp.bfloat16)


def solution(mesh):
    fine = Mesh(mesh.devices.reshape(2, 4, 8, 2, 2), ("yh", "x", "z", "yl", "c"))
    seq, head = ("yh", "x", "z"), ("yl", "c")
    in_specs = (
        P(seq, head),
        P(seq, head),
        P(seq, head),
        P(seq),
        P(None, head),
        P(None, head),
        P(None, head),
        P(),
        P(head, None),
    )
    out_specs = (P(seq + head, None), P(seq, head))
    return jax.shard_map(layer, mesh=fine, in_specs=in_specs, out_specs=out_specs, check_vma=False)
```

```python
from functools import partial
import math

import jax
import jax.numpy as jnp
from jax import lax
from jax.experimental import pallas as pl
from jax.experimental.pallas import tpu as pltpu
from jax.sharding import Mesh, PartitionSpec as P


HEAD_SIZE = 128
T = 192
TP = T + 8
G = 4
R = G * T
ACC = HEAD_SIZE + 8
NB = 16
LOW = -1e30
EMPTY = -1e29
SCALE = HEAD_SIZE**-0.5 * math.log2(math.e)


def shift(x, axis, k):
    n = lax.axis_size(axis)
    return lax.ppermute(x, axis, [((i + k) % n, i) for i in range(n)])


def rounded(x):
    return x.astype(jnp.bfloat16).astype(jnp.float32)


def spec(space=pltpu.VMEM):
    return pl.BlockSpec(memory_space=space)


def params():
    return pltpu.CompilerParams(vmem_limit_bytes=24 << 20)


def pack_body(offset, q, k, v, kv_mine, kv_other, q_mine, q_other, sems):
    yh = lax.axis_index("yh")
    copies = []

    def copy(source, width, head, target, at):
        cols = pl.ds(pl.multiple_of(head * width, width), width)
        copies.append(
            pltpu.make_async_copy(
                source.at[:, cols], target.at[0:T, at : at + width], sems.at[len(copies)]
            )
        )
        copies[-1].start()

    for kv, qq, head in ((kv_other, q_other, 1 - yh), (kv_mine, q_mine, yh)):
        copy(k, HEAD_SIZE, head, kv, 0)
        copy(v, HEAD_SIZE, head, kv, HEAD_SIZE)
        copy(q, 512, head, qq, 0)
    tile = jnp.full((8, 512), offset[0], jnp.int32).astype(jnp.float32).astype(jnp.bfloat16)
    for kv, qq in ((kv_mine, q_mine), (kv_other, q_other)):
        kv[T:TP, :] = tile[:, :256]
        qq[T:TP, :] = tile
    for c in copies:
        c.wait()


def pack(offset, q, k, v):
    return pl.pallas_call(
        pack_body,
        in_specs=[spec(pltpu.SMEM)] + [spec(pltpu.HBM)] * 3,
        out_specs=[spec()] * 4,
        out_shape=[
            jax.ShapeDtypeStruct((TP, width), jnp.bfloat16) for width in (256, 256, 512, 512)
        ],
        scratch_shapes=[pltpu.SemaphoreType.DMA((6,))],
        compiler_params=params(),
        name="pack",
    )(offset, q, k, v)


def dec_step(q, blocks, acc, top, total):
    scores = []
    high = top
    for k, _, seen in blocks:
        s = lax.dot_general(
            q, k, (((1,), (1,)), ((), ())), preferred_element_type=jnp.float32
        )
        s = jnp.where(seen, s * SCALE, LOW)
        scores.append(s)
        high = jnp.maximum(high, rounded(jnp.max(s, axis=1, keepdims=True)))
    factor = jnp.exp2(top - high)
    total, acc = total * factor, acc * factor
    for s, (_, v, seen) in zip(scores, blocks):
        w = jnp.where(seen, jnp.exp2(s - high), 0.0)
        total = total + jnp.sum(w, axis=1, keepdims=True)
        acc = acc + jnp.dot(w.astype(jnp.bfloat16), v, preferred_element_type=jnp.float32)
    return acc, high, total


def sort_blocks(pieces, kv, table, limit):
    keys = lax.broadcasted_iota(jnp.int32, (32, T), 1)
    where = []
    for ref in pieces:
        for at in (0, TP):
            tag = ref[at + T : at + TP, 0:128].astype(jnp.float32)
            where.append((ref, at, jnp.max(tag).astype(jnp.int32)))
    blocks = []
    for ref, at, pos in where:
        rank = sum((other < pos).astype(jnp.int32) for _, _, other in where)
        block = ref[at : at + T, :]
        kv[pl.ds(pl.multiple_of(rank * T, T), T), :] = block
        table[rank] = pos
        blocks.append((block[:, :HEAD_SIZE], block[:, HEAD_SIZE:], keys + pos * T < limit))
    return blocks


def early_body(dq, sk, sv, dpos, *refs):
    pieces, state = refs[:-1], refs[-1]
    q = dq[...]
    limit = dpos[:, 0:1]
    keys = lax.broadcasted_iota(jnp.int32, (32, T), 1)
    blocks = []
    for ref in pieces:
        for at in (0, TP):
            pos = ref[at + T : at + T + 1, 0:1].astype(jnp.float32).astype(jnp.int32)
            block = ref[at : at + T, :]
            blocks.append((block[:, :HEAD_SIZE], block[:, HEAD_SIZE:], keys + pos * T < limit))
    own = lax.broadcasted_iota(jnp.int32, (32, 1), 0) < 8
    score = jnp.sum(q.astype(jnp.float32) * sk[...].astype(jnp.float32), axis=1, keepdims=True)
    score = jnp.where(own, score * SCALE, LOW)
    top = rounded(score)
    weight = jnp.where(own, jnp.exp2(score - top), 0.0)
    acc = rounded(weight) * sv[...].astype(jnp.float32)
    acc, top, total = dec_step(q, blocks, acc, top, weight)
    state[0:32, :] = acc
    state[32:64, :] = jnp.broadcast_to(top, (32, HEAD_SIZE))
    state[64:96, :] = jnp.broadcast_to(total, (32, HEAD_SIZE))


def early(small, pieces):
    return pl.pallas_call(
        early_body,
        in_specs=[spec()] * (len(small) + len(pieces)),
        out_specs=spec(),
        out_shape=jax.ShapeDtypeStruct((96, HEAD_SIZE), jnp.float32),
        compiler_params=params(),
        name="early",
    )(*small, *pieces)


def gather_body(early_blocks, dq, state, dpos, *refs):
    pieces, (kv, table, dec) = refs[:-3], refs[-3:]
    blocks = sort_blocks(pieces, kv, table, dpos[:, 0:1])[early_blocks:]
    acc, top, total = dec_step(
        dq[...], blocks, state[0:32, :], state[32:64, 0:1], state[64:96, 0:1]
    )
    rows = lax.broadcasted_iota(jnp.int32, (8, R), 0)
    top = jnp.broadcast_to(top, (32, HEAD_SIZE))
    total = jnp.broadcast_to(total, (32, HEAD_SIZE))
    for n in range(8):

        def row(a):
            parts = [a[n * G + h : n * G + h + 1, :] for h in range(G)]
            flat = jnp.concatenate(parts + [jnp.zeros((1, 256), jnp.float32)], axis=1)
            return jnp.broadcast_to(flat, (8, R))

        tile = jnp.where(rows == 2, row(acc), 0.0)
        tile = jnp.where(rows == 3, row(top), tile)
        tile = jnp.where(rows == 4, row(total), tile)
        dec[n] = tile


def gather(early_blocks, small, pieces):
    return pl.pallas_call(
        partial(gather_body, early_blocks),
        in_specs=[spec()] * (len(small) + len(pieces)),
        out_specs=[spec(), spec(pltpu.SMEM), spec()],
        out_shape=[
            jax.ShapeDtypeStruct((NB * T, 256), jnp.bfloat16),
            jax.ShapeDtypeStruct((NB,), jnp.int32),
            jax.ShapeDtypeStruct((8, 8, R), jnp.float32),
        ],
        compiler_params=params(),
        name="gather",
    )(*small, *pieces)


W = 256
SPREAD = 60.0


def attend_body(groups, table, *refs):
    n = len(groups)
    queries, (kv, dec), outs = refs[:n], refs[n : n + 2], refs[n + 2 : 2 * n + 2]
    qs, acc, stat, positions, again = refs[2 * n + 2 :]
    for i, q in enumerate(queries):
        for b in range(2):
            at = b * TP
            for h in range(G):
                qs[2 * i + b, h * T : (h + 1) * T, :] = q[
                    at : at + T, h * HEAD_SIZE : (h + 1) * HEAD_SIZE
                ]
            tag = q[at + T : at + TP, 0:128].astype(jnp.float32)
            positions[2 * i + b] = jnp.max(tag).astype(jnp.int32)
    rows = lax.broadcasted_iota(jnp.int32, (8, R), 0)
    cols = list(range(0, R, W))

    @pl.loop(0, n)
    def _(turn):
        counts, sames = [], []
        for b in range(2):
            pos = positions[2 * turn + b]
            count = jnp.int32(0)
            same = jnp.int32(0)
            for m in range(NB):
                count = count + (table[m] < pos).astype(jnp.int32)
                same = same + (table[m] == pos).astype(jnp.int32)
            counts.append(count)
            sames.append(same)
        rests = [c + s for c, s in zip(counts, sames)]

        def read(first, blocks, b):
            at = pl.multiple_of(first * T, T)
            k = kv[pl.ds(at, blocks * T), 0:HEAD_SIZE]
            v = kv[pl.ds(at, blocks * T), HEAD_SIZE:]
            scores = [
                lax.dot_general(
                    k,
                    qs[2 * turn + b, c : c + W, :],
                    (((1,), (1,)), ((), ())),
                    preferred_element_type=jnp.float32,
                )
                for c in cols
            ]
            return v, scores

        def apply(v, w):
            return lax.dot_general(
                v,
                w.astype(jnp.bfloat16),
                (((0,), (0,)), ((), ())),
                preferred_element_type=jnp.float32,
            )

        def exact(fours, i):
            reads = []
            for b in range(2):
                first = jnp.minimum(4 * fours[b] + 2 * i, NB - 2)
                live = 4 * fours[b] + 2 * i < rests[b]
                seen = jnp.where(live, (counts[b] - first) * T, -2 * NB * T)
                reads.append((seen, *read(first, 2, b)))
            for n, c in enumerate(cols):
                row = lax.broadcasted_iota(jnp.int32, (1, W), 1) + c
                for edge in (3 * T, 2 * T, T):
                    row = jnp.where(row >= edge, row - edge, row)
                key = lax.broadcasted_iota(jnp.int32, (2 * T, W), 0)
                for b, (seen, v, scores) in enumerate(reads):
                    limit = jnp.where(sames[b] > 0, row, -1) + seen
                    s = jnp.where(key <= limit, scores[n] * SCALE, LOW)
                    old = stat[b, 0:1, c : c + W]
                    high = jnp.maximum(old, rounded(jnp.max(s, axis=0, keepdims=True)))
                    factor = jnp.exp2(old - high)
                    w = jnp.exp2(s - high)
                    stat[b, 0:1, c : c + W] = high
                    stat[b, 1:2, c : c + W] = stat[b, 1:2, c : c + W] * factor + jnp.sum(
                        w, axis=0, keepdims=True
                    )
                    acc[b, :, c : c + W] = acc[b, :, c : c + W] * factor + apply(v, w)

        def quick(first, which):
            reads = [(b, *read(first, 4, b)) for b in which]
            for n, c in enumerate(cols):
                for b, v, scores in reads:
                    s = scores[n] * SCALE
                    w = jnp.exp2(s - stat[b, 0:1, c : c + W])
                    stat[b, 2:3, c : c + W] = jnp.maximum(
                        stat[b, 2:3, c : c + W], jnp.max(s, axis=0, keepdims=True)
                    )
                    stat[b, 1:2, c : c + W] = stat[b, 1:2, c : c + W] + jnp.sum(
                        w, axis=0, keepdims=True
                    )
                    acc[b, :, c : c + W] = acc[b, :, c : c + W] + apply(v, w)

        again[0] = jnp.int32(1)

        @pl.loop(0, 2)
        def _(attempt):
            @pl.when(again[0] == 1)
            def _():
                fours = [
                    jnp.where(attempt == 0, jnp.maximum(rest - 1, 0) // 4, 0) for rest in rests
                ]
                acc[...] = jnp.zeros_like(acc)
                for b in range(2):
                    stat[b] = jnp.where(rows == 1, 0.0, EMPTY)
                left = [(rest - 4 * f + 1) // 2 for rest, f in zip(rests, fours)]

                @pl.loop(0, jnp.maximum(left[0], left[1]))
                def _(i):
                    exact(fours, i)

                both = jnp.minimum(fours[0], fours[1])
                longer = (fours[1] > fours[0]).astype(jnp.int32)

                @pl.loop(0, both)
                def _(i):
                    quick(4 * i, (0, 1))

                @pl.loop(both, jnp.maximum(fours[0], fours[1]))
                def _(i):
                    quick(4 * i, (longer,))

                over = jnp.maximum(
                    jnp.max(stat[0, 2:3, :] - stat[0, 0:1, :]),
                    jnp.max(stat[1, 2:3, :] - stat[1, 0:1, :]),
                )
                again[0] = (over > SPREAD).astype(jnp.int32)

        for i, (out, group) in enumerate(zip(outs, groups)):

            @pl.when(turn == i)
            def _():
                for b in range(2):
                    out[b, 0:HEAD_SIZE, :] = acc[b].astype(jnp.bfloat16)
                    tile = jnp.where(rows < 2, stat[b], dec[2 * group + b])
                    out[b, HEAD_SIZE:, :] = tile.astype(jnp.bfloat16)


def attend_call(table, queries, kv, dec, groups):
    n = len(groups)
    return pl.pallas_call(
        partial(attend_body, groups),
        in_specs=[spec(pltpu.SMEM)] + [spec()] * (n + 2),
        out_specs=[spec()] * n,
        out_shape=[jax.ShapeDtypeStruct((2, ACC, R), jnp.bfloat16)] * n,
        scratch_shapes=[
            pltpu.VMEM((2 * n, R, HEAD_SIZE), jnp.bfloat16),
            pltpu.VMEM((2, HEAD_SIZE, R), jnp.float32),
            pltpu.VMEM((2, 8, R), jnp.float32),
            pltpu.SMEM((2 * n,), jnp.int32),
            pltpu.SMEM((1,), jnp.int32),
        ],
        cost_estimate=pl.CostEstimate(
            flops=2 * n * NB * T * R * HEAD_SIZE * 4,
            bytes_accessed=4 << 20,
            transcendentals=2 * n * NB * T * R,
        ),
        compiler_params=params(),
        name="attend",
    )(table, *queries, kv, dec)


def merge_body(*refs):
    core = lax.axis_index("c")
    parts, outs, turned = refs[:4], refs[4:8], refs[8]
    for b in range(2):
        stats = [p[b, HEAD_SIZE:, :].astype(jnp.float32) for p in parts]
        high = stats[0][0:1, :]
        for s in stats[1:]:
            high = jnp.maximum(high, s[0:1, :])
        factors = [jnp.exp2(s[0:1, :] - high) for s in stats]
        total = sum(f * s[1:2, :] for f, s in zip(factors, stats))
        acc = sum(
            f * p[b, 0:HEAD_SIZE, :].astype(jnp.float32) for f, p in zip(factors, parts)
        )
        flat = acc / total
        for h in range(G):
            head = flat[:, h * T : (h + 1) * T].T
            turned[:, h * HEAD_SIZE : (h + 1) * HEAD_SIZE] = head.astype(jnp.bfloat16)
        high = stats[0][3:4, :512]
        for s in stats[1:]:
            high = jnp.maximum(high, s[3:4, :512])
        factors = [jnp.exp2(s[3:4, :512] - high) for s in stats]
        total = sum(f * s[4:5, :512] for f, s in zip(factors, stats))
        acc = sum(f * s[2:3, :512] for f, s in zip(factors, stats))
        row = jnp.broadcast_to(acc / total, (8, 512)).astype(jnp.bfloat16)
        for other in range(2):
            out = outs[2 * b + other]
            start = core * 48 if other == 0 else (1 - core) * 48
            for half in range(2):
                rows = pl.ds(pl.multiple_of(start + 96 * half, 16), 48)
                out[half * 48 : half * 48 + 48, :] = turned[rows, :]
            out[96:104, :] = row


def merge(parts):
    return pl.pallas_call(
        merge_body,
        in_specs=[spec()] * 4,
        out_specs=[spec()] * 4,
        out_shape=[jax.ShapeDtypeStruct((104, 512), jnp.bfloat16)] * 4,
        scratch_shapes=[pltpu.VMEM((T, 512), jnp.bfloat16)],
        compiler_params=params(),
        name="merge",
    )(*parts)


def fetch_body(source, target, sems):
    copies = []
    for n in range(8):
        rows = pl.ds(n * 128, 128)
        copies.append(pltpu.make_async_copy(source.at[rows], target.at[rows], sems.at[n]))
        copies[-1].start()
    for c in copies:
        c.wait()


def fetch(w):
    return pl.pallas_call(
        fetch_body,
        in_specs=[spec(pltpu.HBM)],
        out_specs=spec(),
        out_shape=jax.ShapeDtypeStruct(w.shape, w.dtype),
        scratch_shapes=[pltpu.SemaphoreType.DMA((8,))],
        compiler_params=params(),
        name="fetch",
    )(w)


def project_body(half, mine, by_pair, by_core, by_both, w, other_w, *refs):
    send, keep = refs[-2:]
    yh, low_here = lax.axis_index("yh"), lax.axis_index("yl") == 0
    here = pl.ds(pl.multiple_of(yh * 512, 512), 512)
    there = pl.ds(pl.multiple_of((1 - yh) * 512, 512), 512)
    for n in range(0, 2048, 512):
        cols = slice(half * 2048 + n, half * 2048 + n + 512)
        result = sum(
            jnp.dot(a[...], b[rows, cols], preferred_element_type=jnp.float32)
            for a, b, rows in (
                (mine, w, here),
                (by_core, other_w, here),
                (by_pair, w, there),
                (by_both, other_w, there),
            )
        )
        low, high, tail = result[:48], result[48:96], result[96:]
        send[:48, n : n + 512] = jnp.where(low_here, high, low).astype(jnp.bfloat16)
        keep[:48, n : n + 512] = jnp.where(low_here, low, high)
        keep[48:, n : n + 512] = tail
    if half == 1:
        tail = jnp.where(low_here, keep[48:49, :], refs[0][48:49, :])
        tail = jnp.where(lax.axis_index("c") == 0, tail[:, :1024], tail[:, 1024:])
        parts = [tail[:, n * 128 : n * 128 + 128] for n in range(8)]
        send[0:8, 2048:] = jnp.concatenate(parts, axis=0).astype(jnp.bfloat16)
        send[8:48, 2048:] = jnp.zeros((40, 128), jnp.bfloat16)


def project(half, *operands):
    return pl.pallas_call(
        partial(project_body, half),
        in_specs=[spec()] * len(operands),
        out_specs=[spec()] * 2,
        out_shape=[
            jax.ShapeDtypeStruct((48, 2048 + 128 * half), jnp.bfloat16),
            jax.ShapeDtypeStruct((56, 2048), jnp.float32),
        ],
        cost_estimate=pl.CostEstimate(
            flops=104 * 2048 * 2048 * 2, bytes_accessed=9 << 20, transcendentals=0
        ),
        compiler_params=params(),
        name="project",
    )(*operands)


def close_body(keep_0, keep_1, arrived_0, arrived_1, layer_out, dec_out):
    for half, (keep, arrived) in enumerate(((keep_0, arrived_0), (keep_1, arrived_1))):
        result = keep[:48, :] + arrived[:, :2048].astype(jnp.float32)
        layer_out[:, half * 2048 : half * 2048 + 2048] = result.astype(jnp.bfloat16)
    tail = jnp.where(lax.axis_index("yl") == 0, keep_0[48:49, :], keep_1[48:49, :])
    tail = jnp.where(lax.axis_index("c") == 0, tail[:, :1024], tail[:, 1024:])
    other = arrived_1[0:8, 2048:].astype(jnp.float32)
    other = jnp.concatenate([other[n : n + 1, :] for n in range(8)], axis=1)
    dec_out[...] = (tail + other).astype(jnp.bfloat16)


def close(*operands):
    return pl.pallas_call(
        close_body,
        in_specs=[spec()] * 4,
        out_specs=[spec()] * 2,
        out_shape=[
            jax.ShapeDtypeStruct((48, 4096), jnp.bfloat16),
            jax.ShapeDtypeStruct((1, 1024), jnp.bfloat16),
        ],
        compiler_params=params(),
        name="close",
    )(*operands)


def layer(q, k, v, span_offset, appended_q, appended_k, appended_v, dec_pos, out_weight):
    yh, x, z = (lax.axis_index(a) for a in ("yh", "x", "z"))
    kv_mine, kv_other, q_mine, q_other = pack(span_offset, q, k, v)
    kv_pair = jnp.concatenate([kv_mine, shift(kv_other, "yh", 1)], axis=0)
    q_pair = jnp.concatenate([q_mine, shift(q_other, "yh", 1)], axis=0)

    other_weight = fetch(shift(out_weight, "c", 1))

    f1, b1 = shift(kv_pair, "z", 1), shift(kv_pair, "z", -1)
    f2, b2 = shift(f1, "z", 1), shift(b1, "z", -1)
    f2, b2, appended_q, appended_k, appended_v, dec_pos = lax.optimization_barrier(
        (f2, b2, appended_q, appended_k, appended_v, dec_pos)
    )
    tokens = jnp.stack(
        [
            jnp.bitwise_xor(yh, b) * 32 + ((x + g) % 4) * 8 + z
            for g in range(4)
            for b in range(2)
        ]
    ).astype(jnp.int32)
    pick = (tokens[:, None] == jnp.arange(64, dtype=jnp.int32)[None, :]).astype(jnp.bfloat16)

    def rows_of(a):
        w = a.shape[1] // 2
        a = jnp.where(yh == 0, a[:, :w], a[:, w:])
        return jnp.dot(pick, a, preferred_element_type=jnp.float32).astype(jnp.bfloat16)

    dq = rows_of(appended_q).reshape(32, HEAD_SIZE)
    sk = jnp.repeat(rows_of(appended_k), G, axis=0)
    sv = jnp.repeat(rows_of(appended_v), G, axis=0)
    dpos = jnp.sum(jnp.where(tokens[:, None] == jnp.arange(64)[None, :], dec_pos[None, :], 0), axis=1)
    dpos = jnp.broadcast_to(jnp.repeat(dpos, G)[:, None], (32, 128)).astype(jnp.int32)

    groups = [q_pair, shift(q_pair, "x", 1), shift(q_pair, "x", 2), shift(q_pair, "x", -1)]
    state = early([dq, sk, sv, dpos], [kv_pair, f1, b1])
    f3, b3 = shift(f2, "z", 1), shift(b2, "z", -1)
    f4 = shift(f3, "z", 1)
    kv, table, dec = gather(6, [dq, state, dpos], [kv_pair, f1, b1, f2, b2, f3, b3, f4])
    table, other_weight = lax.optimization_barrier((table, other_weight))
    (far,) = attend_call(table, [groups[2]], kv, dec, [2])
    table, far = lax.optimization_barrier((table, far))
    back2 = shift(far, "x", 2)
    ahead, behind = attend_call(table, [groups[1], groups[3]], kv, dec, [1, 3])
    table, ahead, behind = lax.optimization_barrier((table, ahead, behind))
    back1 = shift(ahead, "x", -1)
    back3 = shift(behind, "x", 1)
    (own,) = attend_call(table, [groups[0]], kv, dec, [0])

    mine, by_core, by_pair, by_both = merge([own, back1, back2, back3])
    by_core = shift(by_core, "c", 1)
    by_pair = shift(by_pair, "yh", 1)
    by_both = lax.ppermute(by_both, ("yh", "c"), [(i, 3 - i) for i in range(4)])
    pieces = (mine, by_pair, by_core, by_both)
    send_0, keep_0 = project(0, *pieces, out_weight, other_weight)
    send_0, keep_0, *pieces = lax.optimization_barrier((send_0, keep_0, *pieces))
    arrived_0 = shift(send_0, "yl", 1)
    send_1, keep_1 = project(1, *pieces, out_weight, other_weight, keep_0)
    arrived_1 = shift(send_1, "yl", 1)
    return close(keep_0, keep_1, arrived_0, arrived_1)


def solution(mesh):
    fine = Mesh(mesh.devices.reshape(2, 4, 8, 2, 2), ("yh", "x", "z", "yl", "c"))
    seq, head = ("yh", "x", "z"), ("yl", "c")
    in_specs = (
        P(seq, head),
        P(seq, head),
        P(seq, head),
        P(seq),
        P(None, head),
        P(None, head),
        P(None, head),
        P(),
        P(head, None),
    )
    out_specs = (P(seq + head, None), P(seq, head))
    return jax.shard_map(layer, mesh=fine, in_specs=in_specs, out_specs=out_specs, check_vma=False)
```

```python
from functools import partial
import math

import jax
import jax.numpy as jnp
from jax import lax
from jax.experimental import pallas as pl
from jax.experimental.pallas import tpu as pltpu
from jax.sharding import Mesh, PartitionSpec as P


HEAD_SIZE = 128
T = 192
TP = T + 8
G = 4
R = G * T
ACC = HEAD_SIZE + 8
NB = 16
LOW = -1e30
EMPTY = -1e29
SCALE = HEAD_SIZE**-0.5 * math.log2(math.e)


def shift(x, axis, k):
    n = lax.axis_size(axis)
    return lax.ppermute(x, axis, [((i + k) % n, i) for i in range(n)])


def rounded(x):
    return x.astype(jnp.bfloat16).astype(jnp.float32)


def spec(space=pltpu.VMEM):
    return pl.BlockSpec(memory_space=space)


def params():
    return pltpu.CompilerParams(vmem_limit_bytes=24 << 20)


def pack_body(offset, *refs):
    arrays, (mine, other, sems) = refs[:-3], refs[-3:]
    count = len(arrays)
    yh = lax.axis_index("yh")
    width = mine.shape[1] // count
    copies = []
    for target, head in ((other, 1 - yh), (mine, yh)):
        cols = pl.ds(pl.multiple_of(head * width, width), width)
        for n, a in enumerate(arrays):
            copies.append(
                pltpu.make_async_copy(
                    a.at[:, cols],
                    target.at[0:T, n * width : (n + 1) * width],
                    sems.at[len(copies)],
                )
            )
            copies[-1].start()
    tile = jnp.full((8, mine.shape[1]), offset[0], jnp.int32)
    tile = tile.astype(jnp.float32).astype(jnp.bfloat16)
    for target in (mine, other):
        target[T:TP, :] = tile
    for c in copies:
        c.wait()


def pack(offset, *arrays):
    width = sum(a.shape[1] for a in arrays) // 2
    return pl.pallas_call(
        pack_body,
        in_specs=[spec(pltpu.SMEM)] + [spec(pltpu.HBM)] * len(arrays),
        out_specs=[spec()] * 2,
        out_shape=[jax.ShapeDtypeStruct((TP, width), jnp.bfloat16)] * 2,
        scratch_shapes=[pltpu.SemaphoreType.DMA((2 * len(arrays),))],
        compiler_params=params(),
        name="pack",
    )(offset, *arrays)


def dec_step(q, blocks, acc, top, total):
    scores = []
    high = top
    for k, _, seen in blocks:
        s = lax.dot_general(
            q, k, (((1,), (1,)), ((), ())), preferred_element_type=jnp.float32
        )
        s = jnp.where(seen, s * SCALE, LOW)
        scores.append(s)
        high = jnp.maximum(high, rounded(jnp.max(s, axis=1, keepdims=True)))
    factor = jnp.exp2(top - high)
    total, acc = total * factor, acc * factor
    for s, (_, v, seen) in zip(scores, blocks):
        w = jnp.where(seen, jnp.exp2(s - high), 0.0)
        total = total + jnp.sum(w, axis=1, keepdims=True)
        acc = acc + jnp.dot(w.astype(jnp.bfloat16), v, preferred_element_type=jnp.float32)
    return acc, high, total


def sort_blocks(pieces, kv, table, limit):
    keys = lax.broadcasted_iota(jnp.int32, (32, T), 1)
    where = []
    for ref in pieces:
        for at in (0, TP):
            tag = ref[at + T : at + TP, 0:128].astype(jnp.float32)
            where.append((ref, at, jnp.max(tag).astype(jnp.int32)))
    blocks = []
    for ref, at, pos in where:
        rank = sum((other < pos).astype(jnp.int32) for _, _, other in where)
        block = ref[at : at + T, :]
        kv[pl.ds(pl.multiple_of(rank * T, T), T), :] = block
        table[rank] = pos
        blocks.append((block[:, :HEAD_SIZE], block[:, HEAD_SIZE:], keys + pos * T < limit))
    return blocks


def early_body(dq, sk, sv, dpos, *refs):
    pieces, state = refs[:-1], refs[-1]
    q = dq[...]
    limit = dpos[:, 0:1]
    keys = lax.broadcasted_iota(jnp.int32, (32, T), 1)
    blocks = []
    for ref in pieces:
        for at in (0, TP):
            pos = ref[at + T : at + T + 1, 0:1].astype(jnp.float32).astype(jnp.int32)
            block = ref[at : at + T, :]
            blocks.append((block[:, :HEAD_SIZE], block[:, HEAD_SIZE:], keys + pos * T < limit))
    own = lax.broadcasted_iota(jnp.int32, (32, 1), 0) < 8
    score = jnp.sum(q.astype(jnp.float32) * sk[...].astype(jnp.float32), axis=1, keepdims=True)
    score = jnp.where(own, score * SCALE, LOW)
    top = rounded(score)
    weight = jnp.where(own, jnp.exp2(score - top), 0.0)
    acc = rounded(weight) * sv[...].astype(jnp.float32)
    acc, top, total = dec_step(q, blocks, acc, top, weight)
    state[0:32, :] = acc
    state[32:64, :] = jnp.broadcast_to(top, (32, HEAD_SIZE))
    state[64:96, :] = jnp.broadcast_to(total, (32, HEAD_SIZE))


def early(small, pieces):
    return pl.pallas_call(
        early_body,
        in_specs=[spec()] * (len(small) + len(pieces)),
        out_specs=spec(),
        out_shape=jax.ShapeDtypeStruct((96, HEAD_SIZE), jnp.float32),
        compiler_params=params(),
        name="early",
    )(*small, *pieces)


def gather_body(early_blocks, dq, state, dpos, *refs):
    pieces, (kv, table, dec) = refs[:-3], refs[-3:]
    blocks = sort_blocks(pieces, kv, table, dpos[:, 0:1])[early_blocks:]
    acc, top, total = dec_step(
        dq[...], blocks, state[0:32, :], state[32:64, 0:1], state[64:96, 0:1]
    )
    rows = lax.broadcasted_iota(jnp.int32, (8, R), 0)
    top = jnp.broadcast_to(top, (32, HEAD_SIZE))
    total = jnp.broadcast_to(total, (32, HEAD_SIZE))
    for n in range(8):

        def row(a):
            parts = [a[n * G + h : n * G + h + 1, :] for h in range(G)]
            flat = jnp.concatenate(parts + [jnp.zeros((1, 256), jnp.float32)], axis=1)
            return jnp.broadcast_to(flat, (8, R))

        tile = jnp.where(rows == 2, row(acc), 0.0)
        tile = jnp.where(rows == 3, row(top), tile)
        tile = jnp.where(rows == 4, row(total), tile)
        dec[n] = tile


def gather(early_blocks, small, pieces):
    return pl.pallas_call(
        partial(gather_body, early_blocks),
        in_specs=[spec()] * (len(small) + len(pieces)),
        out_specs=[spec(), spec(pltpu.SMEM), spec()],
        out_shape=[
            jax.ShapeDtypeStruct((NB * T, 256), jnp.bfloat16),
            jax.ShapeDtypeStruct((NB,), jnp.int32),
            jax.ShapeDtypeStruct((8, 8, R), jnp.float32),
        ],
        compiler_params=params(),
        name="gather",
    )(*small, *pieces)


W = 256
SPREAD = 60.0


def attend_body(groups, table, *refs):
    n = len(groups)
    queries, (kv, dec), outs = refs[:n], refs[n : n + 2], refs[n + 2 : 2 * n + 2]
    qs, acc, stat, positions, again = refs[2 * n + 2 :]
    for i, q in enumerate(queries):
        for b in range(2):
            at = b * TP
            for h in range(G):
                qs[2 * i + b, h * T : (h + 1) * T, :] = q[
                    at : at + T, h * HEAD_SIZE : (h + 1) * HEAD_SIZE
                ]
            tag = q[at + T : at + TP, 0:128].astype(jnp.float32)
            positions[2 * i + b] = jnp.max(tag).astype(jnp.int32)
    rows = lax.broadcasted_iota(jnp.int32, (8, R), 0)
    cols = list(range(0, R, W))

    @pl.loop(0, n)
    def _(turn):
        counts, sames = [], []
        for b in range(2):
            pos = positions[2 * turn + b]
            count = jnp.int32(0)
            same = jnp.int32(0)
            for m in range(NB):
                count = count + (table[m] < pos).astype(jnp.int32)
                same = same + (table[m] == pos).astype(jnp.int32)
            counts.append(count)
            sames.append(same)
        rests = [c + s for c, s in zip(counts, sames)]

        def read(first, blocks, b):
            at = pl.multiple_of(first * T, T)
            k = kv[pl.ds(at, blocks * T), 0:HEAD_SIZE]
            v = kv[pl.ds(at, blocks * T), HEAD_SIZE:]
            scores = [
                lax.dot_general(
                    k,
                    qs[2 * turn + b, c : c + W, :],
                    (((1,), (1,)), ((), ())),
                    preferred_element_type=jnp.float32,
                )
                for c in cols
            ]
            return v, scores

        def apply(v, w):
            return lax.dot_general(
                v,
                w.astype(jnp.bfloat16),
                (((0,), (0,)), ((), ())),
                preferred_element_type=jnp.float32,
            )

        def exact(fours, i):
            reads = []
            for b in range(2):
                first = jnp.minimum(4 * fours[b] + 2 * i, NB - 2)
                live = 4 * fours[b] + 2 * i < rests[b]
                seen = jnp.where(live, (counts[b] - first) * T, -2 * NB * T)
                reads.append((seen, *read(first, 2, b)))
            for n, c in enumerate(cols):
                row = lax.broadcasted_iota(jnp.int32, (1, W), 1) + c
                for edge in (3 * T, 2 * T, T):
                    row = jnp.where(row >= edge, row - edge, row)
                key = lax.broadcasted_iota(jnp.int32, (2 * T, W), 0)
                for b, (seen, v, scores) in enumerate(reads):
                    limit = jnp.where(sames[b] > 0, row, -1) + seen
                    s = jnp.where(key <= limit, scores[n] * SCALE, LOW)
                    old = stat[b, 0:1, c : c + W]
                    high = jnp.maximum(old, rounded(jnp.max(s, axis=0, keepdims=True)))
                    factor = jnp.exp2(old - high)
                    w = jnp.exp2(s - high)
                    stat[b, 0:1, c : c + W] = high
                    stat[b, 1:2, c : c + W] = stat[b, 1:2, c : c + W] * factor + jnp.sum(
                        w, axis=0, keepdims=True
                    )
                    acc[b, :, c : c + W] = acc[b, :, c : c + W] * factor + apply(v, w)

        def quick(first, which):
            reads = [(b, *read(first, 4, b)) for b in which]
            for n, c in enumerate(cols):
                for b, v, scores in reads:
                    s = scores[n] * SCALE
                    w = jnp.exp2(s - stat[b, 0:1, c : c + W])
                    stat[b, 2:3, c : c + W] = jnp.maximum(
                        stat[b, 2:3, c : c + W], jnp.max(s, axis=0, keepdims=True)
                    )
                    stat[b, 1:2, c : c + W] = stat[b, 1:2, c : c + W] + jnp.sum(
                        w, axis=0, keepdims=True
                    )
                    acc[b, :, c : c + W] = acc[b, :, c : c + W] + apply(v, w)

        again[0] = jnp.int32(1)

        @pl.loop(0, 2)
        def _(attempt):
            @pl.when(again[0] == 1)
            def _():
                fours = [
                    jnp.where(attempt == 0, jnp.maximum(rest - 1, 0) // 4, 0) for rest in rests
                ]
                acc[...] = jnp.zeros_like(acc)
                for b in range(2):
                    stat[b] = jnp.where(rows == 1, 0.0, EMPTY)
                left = [(rest - 4 * f + 1) // 2 for rest, f in zip(rests, fours)]

                @pl.loop(0, jnp.maximum(left[0], left[1]))
                def _(i):
                    exact(fours, i)

                both = jnp.minimum(fours[0], fours[1])
                longer = (fours[1] > fours[0]).astype(jnp.int32)

                @pl.loop(0, both)
                def _(i):
                    quick(4 * i, (0, 1))

                @pl.loop(both, jnp.maximum(fours[0], fours[1]))
                def _(i):
                    quick(4 * i, (longer,))

                over = jnp.maximum(
                    jnp.max(stat[0, 2:3, :] - stat[0, 0:1, :]),
                    jnp.max(stat[1, 2:3, :] - stat[1, 0:1, :]),
                )
                again[0] = (over > SPREAD).astype(jnp.int32)

        for i, (out, group) in enumerate(zip(outs, groups)):

            @pl.when(turn == i)
            def _():
                for b in range(2):
                    out[b, 0:HEAD_SIZE, :] = acc[b].astype(jnp.bfloat16)
                    tile = jnp.where(rows < 2, stat[b], dec[2 * group + b])
                    out[b, HEAD_SIZE:, :] = tile.astype(jnp.bfloat16)


def attend_call(table, queries, kv, dec, groups):
    n = len(groups)
    return pl.pallas_call(
        partial(attend_body, groups),
        in_specs=[spec(pltpu.SMEM)] + [spec()] * (n + 2),
        out_specs=[spec()] * n,
        out_shape=[jax.ShapeDtypeStruct((2, ACC, R), jnp.bfloat16)] * n,
        scratch_shapes=[
            pltpu.VMEM((2 * n, R, HEAD_SIZE), jnp.bfloat16),
            pltpu.VMEM((2, HEAD_SIZE, R), jnp.float32),
            pltpu.VMEM((2, 8, R), jnp.float32),
            pltpu.SMEM((2 * n,), jnp.int32),
            pltpu.SMEM((1,), jnp.int32),
        ],
        cost_estimate=pl.CostEstimate(
            flops=2 * n * NB * T * R * HEAD_SIZE * 4,
            bytes_accessed=4 << 20,
            transcendentals=2 * n * NB * T * R,
        ),
        compiler_params=params(),
        name="attend",
    )(table, *queries, kv, dec)


def merge_body(*refs):
    core = lax.axis_index("c")
    parts, outs, turned = refs[:4], refs[4:8], refs[8]
    for b in range(2):
        stats = [p[b, HEAD_SIZE:, :].astype(jnp.float32) for p in parts]
        high = stats[0][0:1, :]
        for s in stats[1:]:
            high = jnp.maximum(high, s[0:1, :])
        factors = [jnp.exp2(s[0:1, :] - high) for s in stats]
        total = sum(f * s[1:2, :] for f, s in zip(factors, stats))
        acc = sum(
            f * p[b, 0:HEAD_SIZE, :].astype(jnp.float32) for f, p in zip(factors, parts)
        )
        flat = acc / total
        for h in range(G):
            head = flat[:, h * T : (h + 1) * T].T
            turned[:, h * HEAD_SIZE : (h + 1) * HEAD_SIZE] = head.astype(jnp.bfloat16)
        high = stats[0][3:4, :512]
        for s in stats[1:]:
            high = jnp.maximum(high, s[3:4, :512])
        factors = [jnp.exp2(s[3:4, :512] - high) for s in stats]
        total = sum(f * s[4:5, :512] for f, s in zip(factors, stats))
        acc = sum(f * s[2:3, :512] for f, s in zip(factors, stats))
        row = jnp.broadcast_to(acc / total, (8, 512)).astype(jnp.bfloat16)
        for other in range(2):
            out = outs[2 * b + other]
            start = core * 48 if other == 0 else (1 - core) * 48
            for half in range(2):
                rows = pl.ds(pl.multiple_of(start + 96 * half, 16), 48)
                out[half * 48 : half * 48 + 48, :] = turned[rows, :]
            out[96:104, :] = row


def merge(parts):
    return pl.pallas_call(
        merge_body,
        in_specs=[spec()] * 4,
        out_specs=[spec()] * 4,
        out_shape=[jax.ShapeDtypeStruct((104, 512), jnp.bfloat16)] * 4,
        scratch_shapes=[pltpu.VMEM((T, 512), jnp.bfloat16)],
        compiler_params=params(),
        name="merge",
    )(*parts)


def fetch_body(source, target, sems):
    copies = []
    for n in range(8):
        rows = pl.ds(n * 128, 128)
        copies.append(pltpu.make_async_copy(source.at[rows], target.at[rows], sems.at[n]))
        copies[-1].start()
    for c in copies:
        c.wait()


def fetch(w):
    return pl.pallas_call(
        fetch_body,
        in_specs=[spec(pltpu.HBM)],
        out_specs=spec(),
        out_shape=jax.ShapeDtypeStruct(w.shape, w.dtype),
        scratch_shapes=[pltpu.SemaphoreType.DMA((8,))],
        compiler_params=params(),
        name="fetch",
    )(w)


def project_body(half, mine, by_pair, by_core, by_both, w, other_w, *refs):
    send, keep = refs[-2:]
    yh, low_here = lax.axis_index("yh"), lax.axis_index("yl") == 0
    here = pl.ds(pl.multiple_of(yh * 512, 512), 512)
    there = pl.ds(pl.multiple_of((1 - yh) * 512, 512), 512)
    for n in range(0, 2048, 512):
        cols = slice(half * 2048 + n, half * 2048 + n + 512)
        result = sum(
            jnp.dot(a[...], b[rows, cols], preferred_element_type=jnp.float32)
            for a, b, rows in (
                (mine, w, here),
                (by_core, other_w, here),
                (by_pair, w, there),
                (by_both, other_w, there),
            )
        )
        low, high, tail = result[:48], result[48:96], result[96:]
        send[:48, n : n + 512] = jnp.where(low_here, high, low).astype(jnp.bfloat16)
        keep[:48, n : n + 512] = jnp.where(low_here, low, high)
        keep[48:, n : n + 512] = tail
    if half == 1:
        tail = jnp.where(low_here, keep[48:49, :], refs[0][48:49, :])
        tail = jnp.where(lax.axis_index("c") == 0, tail[:, :1024], tail[:, 1024:])
        parts = [tail[:, n * 128 : n * 128 + 128] for n in range(8)]
        send[0:8, 2048:] = jnp.concatenate(parts, axis=0).astype(jnp.bfloat16)
        send[8:48, 2048:] = jnp.zeros((40, 128), jnp.bfloat16)


def project(half, *operands):
    return pl.pallas_call(
        partial(project_body, half),
        in_specs=[spec()] * len(operands),
        out_specs=[spec()] * 2,
        out_shape=[
            jax.ShapeDtypeStruct((48, 2048 + 128 * half), jnp.bfloat16),
            jax.ShapeDtypeStruct((56, 2048), jnp.float32),
        ],
        cost_estimate=pl.CostEstimate(
            flops=104 * 2048 * 2048 * 2, bytes_accessed=9 << 20, transcendentals=0
        ),
        compiler_params=params(),
        name="project",
    )(*operands)


def close_body(keep_0, keep_1, arrived_0, arrived_1, layer_out, dec_out):
    for half, (keep, arrived) in enumerate(((keep_0, arrived_0), (keep_1, arrived_1))):
        result = keep[:48, :] + arrived[:, :2048].astype(jnp.float32)
        layer_out[:, half * 2048 : half * 2048 + 2048] = result.astype(jnp.bfloat16)
    tail = jnp.where(lax.axis_index("yl") == 0, keep_0[48:49, :], keep_1[48:49, :])
    tail = jnp.where(lax.axis_index("c") == 0, tail[:, :1024], tail[:, 1024:])
    other = arrived_1[0:8, 2048:].astype(jnp.float32)
    other = jnp.concatenate([other[n : n + 1, :] for n in range(8)], axis=1)
    dec_out[...] = (tail + other).astype(jnp.bfloat16)


def close(*operands):
    return pl.pallas_call(
        close_body,
        in_specs=[spec()] * 4,
        out_specs=[spec()] * 2,
        out_shape=[
            jax.ShapeDtypeStruct((48, 4096), jnp.bfloat16),
            jax.ShapeDtypeStruct((1, 1024), jnp.bfloat16),
        ],
        compiler_params=params(),
        name="close",
    )(*operands)


def layer(q, k, v, span_offset, appended_q, appended_k, appended_v, dec_pos, out_weight):
    yh, x, z = (lax.axis_index(a) for a in ("yh", "x", "z"))
    kv_mine, kv_other = pack(span_offset, k, v)
    q_mine, q_other = pack(span_offset, q)
    kv_pair = jnp.concatenate([kv_mine, shift(kv_other, "yh", 1)], axis=0)
    q_pair = jnp.concatenate([q_mine, shift(q_other, "yh", 1)], axis=0)

    other_weight = fetch(shift(out_weight, "c", 1))

    f1, b1 = shift(kv_pair, "z", 1), shift(kv_pair, "z", -1)
    f2, b2 = shift(f1, "z", 1), shift(b1, "z", -1)
    f2, b2, appended_q, appended_k, appended_v, dec_pos = lax.optimization_barrier(
        (f2, b2, appended_q, appended_k, appended_v, dec_pos)
    )
    tokens = jnp.stack(
        [
            jnp.bitwise_xor(yh, b) * 32 + ((x + g) % 4) * 8 + z
            for g in range(4)
            for b in range(2)
        ]
    ).astype(jnp.int32)
    pick = (tokens[:, None] == jnp.arange(64, dtype=jnp.int32)[None, :]).astype(jnp.bfloat16)

    def rows_of(a):
        w = a.shape[1] // 2
        a = jnp.where(yh == 0, a[:, :w], a[:, w:])
        return jnp.dot(pick, a, preferred_element_type=jnp.float32).astype(jnp.bfloat16)

    dq = rows_of(appended_q).reshape(32, HEAD_SIZE)
    sk = jnp.repeat(rows_of(appended_k), G, axis=0)
    sv = jnp.repeat(rows_of(appended_v), G, axis=0)
    dpos = jnp.sum(jnp.where(tokens[:, None] == jnp.arange(64)[None, :], dec_pos[None, :], 0), axis=1)
    dpos = jnp.broadcast_to(jnp.repeat(dpos, G)[:, None], (32, 128)).astype(jnp.int32)

    groups = [q_pair, shift(q_pair, "x", 1), shift(q_pair, "x", 2), shift(q_pair, "x", -1)]
    state = early([dq, sk, sv, dpos], [kv_pair, f1, b1])
    f3, b3 = shift(f2, "z", 1), shift(b2, "z", -1)
    f4 = shift(f3, "z", 1)
    kv, table, dec = gather(6, [dq, state, dpos], [kv_pair, f1, b1, f2, b2, f3, b3, f4])
    (far,) = attend_call(table, [groups[2]], kv, dec, [2])
    table, far = lax.optimization_barrier((table, far))
    back2 = shift(far, "x", 2)
    ahead, behind = attend_call(table, [groups[1], groups[3]], kv, dec, [1, 3])
    table, ahead, behind = lax.optimization_barrier((table, ahead, behind))
    back1 = shift(ahead, "x", -1)
    back3 = shift(behind, "x", 1)
    (own,) = attend_call(table, [groups[0]], kv, dec, [0])

    mine, by_core, by_pair, by_both = merge([own, back1, back2, back3])
    by_core = shift(by_core, "c", 1)
    by_pair = shift(by_pair, "yh", 1)
    by_both = lax.ppermute(by_both, ("yh", "c"), [(i, 3 - i) for i in range(4)])
    pieces = (mine, by_pair, by_core, by_both)
    send_0, keep_0 = project(0, *pieces, out_weight, other_weight)
    send_0, keep_0, *pieces = lax.optimization_barrier((send_0, keep_0, *pieces))
    arrived_0 = shift(send_0, "yl", 1)
    send_1, keep_1 = project(1, *pieces, out_weight, other_weight, keep_0)
    arrived_1 = shift(send_1, "yl", 1)
    return close(keep_0, keep_1, arrived_0, arrived_1)


def solution(mesh):
    fine = Mesh(mesh.devices.reshape(2, 4, 8, 2, 2), ("yh", "x", "z", "yl", "c"))
    seq, head = ("yh", "x", "z"), ("yl", "c")
    in_specs = (
        P(seq, head),
        P(seq, head),
        P(seq, head),
        P(seq),
        P(None, head),
        P(None, head),
        P(None, head),
        P(),
        P(head, None),
    )
    out_specs = (P(seq + head, None), P(seq, head))
    return jax.shard_map(layer, mesh=fine, in_specs=in_specs, out_specs=out_specs, check_vma=False)
```
